512 devices in a mesh: bank: 64 (over z, x, core), zero: 8 (over y).
Axes of the slice: x: 4, y: 8, z: 8, core: 2. Of those that a mesh axis runs over, the one named last changes fastest.
Arguments:
- master_down: float32 [64, 1408, 2048], P('bank', None, 'zero'), may hold values from -0.21875 to 0.21875
- second_down: bfloat16 [64, 1408, 2048], P('bank', None, 'zero'), may hold values from -0.078125 to 0.078125
- router_weight: float32 [2048, 64], P('zero', 'bank'), may hold values from -0.125 to 0.125
- router_gain: float32 [2048], P('zero'), may hold values from 0.25 to 1.75
Outputs:
- final_down: bfloat16 [64, 1408, 2048], P('bank')
- scale_down: float32 [64, 1408], P('bank')
- serve_router: bfloat16 [2048, 64], replicated
The draws below stay inside these ranges and needn't reach their ends.
All inputs are finite; a program needn't handle non-finite values.
Results may differ from the reference program's by a relative error of at most 0.001.
Values may be sent and summed in bfloat16 or wider, within the bound.
A program may use at most 64 MiB of HBM per device.

```python
import jax
import jax.numpy as jnp
from jax import lax

EXPERTS = 64
D_MODEL = 2048
D_EXPERT = 1408


def with_spikes(result, own_key, source, target, shards_of, factor):
    owner, partner = [(jnp.arange(result.shape[axis_at]) // (result.shape[axis_at] // shards_of)).reshape([-1 if axis == axis_at else 1 for axis in range(result.ndim)]) for axis_at in (source, target)]
    chosen = jax.random.permutation(own_key, shards_of)[partner]
    strong = (owner == chosen) | (owner == (partner + shards_of // 2) % shards_of)
    return jnp.where(strong, factor * result, result)


def level_of(key, shape, pieces, low, top_value):
    def one(dim, parts):
        draws = jax.random.uniform(jax.random.fold_in(jax.random.fold_in(key, 6), dim), (parts,), jnp.float32, low / len(pieces), top_value / len(pieces))
        return jnp.repeat(jnp.exp(draws), shape[dim] // parts).reshape((-1,) + (1,) * (len(shape) - dim - 1))

    level = one(*pieces[0])
    for cut in pieces[1:]:
        level = level * one(*cut)
    return level


def centred(rng, dims, deviation, most, shards=(), dtype=jnp.bfloat16):
    entries = deviation * jax.random.normal(rng, dims, jnp.float32)
    if shards:
        entries = entries * level_of(rng, dims, shards, -0.22, 0.18)
    return jnp.clip(entries, -most, most).astype(dtype)


def noise_with(own_key, shape, scale, bound, shards, heavy, kind=jnp.bfloat16):
    array = scale * jax.random.normal(own_key, shape, jnp.float32)
    if shards:
        array = array * level_of(own_key, shape, shards, -0.22, 0.18)
    return jnp.clip(with_spikes(array, jax.random.fold_in(own_key, 3), *heavy), -bound, bound).astype(kind)


def setup_inputs(seed: int = 0) -> dict:
    keys = jax.random.split(jax.random.key(seed), 5)
    return {
        "master_down": noise_with(keys[0], (EXPERTS, D_EXPERT, D_MODEL), D_EXPERT ** -0.5, 0.21875, ((0, 64), (2, 8)), (2, 1, 8, 2.0), jnp.float32),
        "second_down": centred(keys[1], (EXPERTS, D_EXPERT, D_MODEL), (D_EXPERT * 4) ** -0.5, 0.078125, ((0, 64), (2, 8))),
        "router_weight": centred(keys[2], (D_MODEL, EXPERTS), D_MODEL ** -0.5, 0.125, ((0, 8), (1, 64)), jnp.float32),
        "router_gain": jnp.clip(1.0 + 0.15 * jax.random.normal(keys[3], (D_MODEL,), jnp.float32), 0.25, 1.75),
    }


def reference(master_down, second_down, router_weight, router_gain):
    merged_down = master_down + second_down.astype(jnp.float32)
    scale_down = jnp.sqrt(lax.optimization_barrier(jnp.sum(merged_down * merged_down, axis=2)))
    final_down = (merged_down / jnp.expand_dims(scale_down, 2)).astype(jnp.bfloat16)
    serve_router = (router_weight * router_gain[:, None]).astype(jnp.bfloat16)
    return (final_down, scale_down, serve_router)
```

```python
import functools

import jax
import jax.numpy as jnp
from jax import lax
from jax.experimental import pallas as pl
from jax.experimental.pallas import tpu as pltpu
from jax.sharding import PartitionSpec as P

MESH = pl.DeviceIdType.MESH
BLOCK = 128
CHUNK = 176
X, CORES = 4, 2


def kernel(
    master, second, weight, gain,
    final, scale, router,
    merged, added, inverse, own_sum, sums, w_v, g_v, part, column, table,
    load_sem, small_sem, local_sem,
    sum_send, sum_recv, ring_send, ring_recv,
    part_send, part_recv, table_send, table_recv,
):
    rows, cols = merged.shape
    zero = lax.axis_size("zero")
    blocks, chunks = rows // BLOCK, rows // CHUNK
    half = chunks // 2
    y, bank = lax.axis_index("zero"), lax.axis_index("bank")
    chip_z, chip_x = bank // (X * CORES), lax.rem(bank // CORES, X)
    depth = lax.axis_size("bank") // (X * CORES)
    core = lax.rem(bank, CORES)

    def at_core(k):
        return bank - core + lax.rem(core + k, CORES)

    def at_x(k):
        return (chip_z * X + lax.rem(chip_x + k, X)) * CORES + core

    def at_z(k):
        return (lax.rem(chip_z + k, depth) * X + chip_x) * CORES + core

    def load(i):
        at = pl.ds(i * BLOCK, BLOCK)
        return (
            pltpu.make_async_copy(master.at[at], merged.at[at], load_sem.at[0, i]),
            pltpu.make_async_copy(second.at[at], added.at[at], load_sem.at[1, i]),
        )

    small = (
        pltpu.make_async_copy(weight, w_v, small_sem.at[0]),
        pltpu.make_async_copy(gain, g_v, small_sem.at[1]),
    )
    for copy in small:
        copy.start()
    for i in range(blocks):
        for copy in load(i):
            copy.start()

    barrier = pltpu.get_barrier_semaphore()
    peers = [{"zero": lax.rem(y + k, zero)} for k in range(1, zero)]
    peers += [{"bank": at_core(1)}]
    peers += [{"bank": at_x(k)} for k in range(1, X)]
    peers += [{"bank": at_z(k)} for k in range(1, depth)]
    for peer in peers:
        pl.semaphore_signal(barrier, inc=1, device_id=peer, device_id_type=MESH)

    for copy in small:
        copy.wait()
    part[...] = (w_v[...] * g_v[...]).astype(jnp.bfloat16).astype(jnp.float32)

    for i in range(blocks):
        at = pl.ds(i * BLOCK, BLOCK)
        for copy in load(i):
            copy.wait()
        value = merged[at] + added[at].astype(jnp.float32)
        merged[at] = value
        square = value * value
        lanes = square[:, :128]
        for j in range(128, cols, 128):
            lanes = lanes + square[:, j : j + 128]
        own_sum[:, at] = jnp.sum(lanes.T, axis=0, keepdims=True)
    sums[y] = own_sum[...]

    pl.semaphore_wait(barrier, len(peers))

    def send_sum(k):
        return pltpu.make_async_remote_copy(
            own_sum, sums.at[y], sum_send.at[k - 1], sum_recv.at[k - 1],
            device_id={"zero": lax.rem(y + k, zero)}, device_id_type=MESH,
        )

    def send_part(k):
        return pltpu.make_async_remote_copy(
            part, column.at[y], part_send.at[k - 1], part_recv.at[k - 1],
            device_id={"zero": lax.rem(y + k, zero)}, device_id_type=MESH,
        )

    for k in (4, 3, 5, 2, 6, 1, 7):
        send_sum(k).start()
    for k in range(1, zero):
        send_part(k).start()
    own_part = pltpu.make_async_copy(part, column.at[y], local_sem.at[0])
    own_part.start()

    for k in range(1, zero):
        send_sum(k).wait_recv()
    total = jnp.sqrt(jnp.sum(sums[...], axis=0))
    scale[...] = total
    own_sum_inverse = 1.0 / total
    for i in range(blocks):
        at = slice(i * BLOCK, (i + 1) * BLOCK)
        inverse[at] = jnp.broadcast_to(own_sum_inverse[:, at], (BLOCK, BLOCK)).T

    def ring(way, hop, c):
        step = 1 if way == 0 else zero - 1
        owner = lax.rem(y + (zero - step) * hop, zero)
        at = final.at[pl.ds(c * CHUNK, CHUNK), pl.ds(pl.multiple_of(owner * cols, cols), cols)]
        return pltpu.make_async_remote_copy(
            at, at, ring_send.at[way, hop, c], ring_recv.at[way, hop, c],
            device_id={"zero": lax.rem(y + step, zero)}, device_id_type=MESH,
        )

    mine = pl.ds(pl.multiple_of(y * cols, cols), cols)

    def own(c, _):
        at = pl.ds(pl.multiple_of(c * CHUNK, CHUNK), CHUNK)
        wide = jnp.concatenate([inverse[at]] * (cols // 128), axis=1)
        final[at, mine] = (merged[at] * wide).astype(jnp.bfloat16)

        @pl.when(c > 0)
        def _():
            ring(0, 0, c - 1).start()
            ring(1, 0, c - 1).start()

        return 0

    lax.fori_loop(0, chunks, own, 0)
    ring(0, 0, chunks - 1).start()
    ring(1, 0, chunks - 1).start()

    own_part.wait()
    for k in range(1, zero):
        send_part(k).wait_recv()

    def send_table(sem, rows_at, count, peer):
        at = table.at[pl.ds(rows_at, count)]
        return pltpu.make_async_remote_copy(
            at, at, table_send.at[sem], table_recv.at[sem],
            device_id={"bank": peer}, device_id_type=MESH,
        )

    own_row = pltpu.make_async_copy(column, table.at[bank], local_sem.at[1])
    own_row.start()
    own_row.wait()
    stages = [
        [send_table(0, bank, 1, at_core(1))],
        [send_table(k, bank - core, CORES, at_x(k)) for k in range(1, X)],
        [send_table(X - 1 + k, chip_z * X * CORES, X * CORES, at_z(k)) for k in range(1, depth)],
    ]

    def table_stage(s):
        if s:
            for copy in stages[s - 1]:
                copy.wait_recv()
        if s < len(stages):
            for copy in stages[s]:
                copy.start()
        else:
            width = part.shape[1]
            for j in range(zero):
                router[:, j * width : (j + 1) * width] = table[:, j, 0, :].astype(jnp.bfloat16)

    def relay(hop, ways, first, last):
        def step(c, _):
            for way in (0, 1):
                ring(way, hop - 1, c).wait_recv()
                if way in ways:
                    ring(way, hop, c).start()
            return 0

        lax.fori_loop(first, last, step, 0)

    table_stage(0)
    relay(1, (0, 1), 0, half)
    table_stage(1)
    relay(1, (0, 1), half, chunks)
    table_stage(2)
    relay(2, (0, 1), 0, chunks)
    table_stage(3)
    relay(3, (0,), 0, half)
    relay(3, (1,), half, chunks)

    def last_cw(c, _):
        ring(0, 3, c).wait_recv()
        ring(1, 3, c + half).wait_recv()
        return 0

    lax.fori_loop(0, half, last_cw, 0)

    def sent(c, _):
        for hop in range(3):
            for way in (0, 1):
                ring(way, hop, c).wait_send()
        return 0

    lax.fori_loop(0, chunks, sent, 0)

    def sent_last(c, _):
        ring(0, 3, c).wait_send()
        ring(1, 3, c + half).wait_send()
        return 0

    lax.fori_loop(0, half, sent_last, 0)
    for k in range(1, zero):
        send_sum(k).wait_send()
        send_part(k).wait_send()
    for stage in stages:
        for copy in stage:
            copy.wait_send()


def in_hbm(value):
    return pltpu.with_memory_space_constraint(value, pltpu.HBM)


def body(master_down, second_down, router_weight, router_gain):
    _, rows, cols = master_down.shape
    width = router_weight.shape[0]
    zero, banks = lax.axis_size("zero"), lax.axis_size("bank")
    blocks, chunks = rows // BLOCK, rows // CHUNK
    depth = banks // (X * CORES)
    f32, vmem, dma = jnp.float32, pltpu.VMEM, pltpu.SemaphoreType.DMA
    final, scale, router = pl.pallas_call(
        kernel,
        out_shape=(
            jax.ShapeDtypeStruct((rows, zero * cols), jnp.bfloat16),
            jax.ShapeDtypeStruct((1, rows), f32),
            jax.ShapeDtypeStruct((banks, zero * width), jnp.bfloat16),
        ),
        in_specs=[pl.BlockSpec(memory_space=pltpu.HBM)] * 4,
        out_specs=[pl.BlockSpec(memory_space=vmem)] * 3,
        scratch_shapes=[
            vmem((rows, cols), f32),
            vmem((rows, cols), jnp.bfloat16),
            vmem((rows, 128), f32),
            vmem((1, rows), f32),
            vmem((zero, 1, rows), f32),
            vmem((1, width), f32),
            vmem((1, width), f32),
            vmem((1, width), f32),
            vmem((zero, 1, width), f32),
            vmem((banks, zero, 1, width), f32),
            dma((2, blocks)),
            dma((2,)),
            dma((2,)),
            dma((zero - 1,)),
            dma((zero - 1,)),
            dma((2, 4, chunks)),
            dma((2, 4, chunks)),
            dma((zero - 1,)),
            dma((zero - 1,)),
            dma((X - 1 + depth,)),
            dma((X - 1 + depth,)),
        ],
        compiler_params=pltpu.CompilerParams(
            collective_id=0, has_side_effects=True, vmem_limit_bytes=40 * 2**20
        ),
        name="gather",
    )(
        in_hbm(master_down.reshape(rows, cols)),
        in_hbm(second_down.reshape(rows, cols)),
        in_hbm(router_weight.reshape(1, width)),
        in_hbm(router_gain.reshape(1, width)),
    )
    return final.reshape(1, rows, zero * cols), scale, router.T


def solution(mesh):
    return jax.shard_map(
        body,
        mesh=mesh,
        in_specs=(P("bank", None, "zero"), P("bank", None, "zero"), P("zero", "bank"), P("zero")),
        out_specs=(P("bank", None, None), P("bank", None), P()),
        check_vma=False,
    )
```

```python
import functools

import jax
import jax.numpy as jnp
from jax import lax
from jax.experimental import pallas as pl
from jax.experimental.pallas import tpu as pltpu
from jax.sharding import PartitionSpec as P

MESH = pl.DeviceIdType.MESH
BLOCK = 128
CHUNK = 88
EARLY = 1
X, CORES = 4, 2


def kernel(
    master, second, weight, gain,
    final, scale, router,
    merged, added, inverse, own_sum, sums, w_v, g_v, part, column, table, early,
    ready, opened, early_send, early_recv, load_sem, small_sem, local_sem,
    sum_send, sum_recv, ring_send, ring_recv,
    part_send, part_recv, table_send, table_recv,
):
    rows, cols = merged.shape
    zero = lax.axis_size("zero")
    blocks, chunks = rows // BLOCK, rows // CHUNK
    half = chunks // 2
    y, bank = lax.axis_index("zero"), lax.axis_index("bank")
    chip_z, chip_x = bank // (X * CORES), lax.rem(bank // CORES, X)
    depth = lax.axis_size("bank") // (X * CORES)
    core = lax.rem(bank, CORES)

    def at_core(k):
        return bank - core + lax.rem(core + k, CORES)

    def at_x(k):
        return (chip_z * X + lax.rem(chip_x + k, X)) * CORES + core

    def at_z(k):
        return (lax.rem(chip_z + k, depth) * X + chip_x) * CORES + core

    def load(i):
        at = pl.ds(i * BLOCK, BLOCK)
        return (
            pltpu.make_async_copy(master.at[at], merged.at[at], load_sem.at[0, i]),
            pltpu.make_async_copy(second.at[at], added.at[at], load_sem.at[1, i]),
        )

    small = (
        pltpu.make_async_copy(weight, w_v, small_sem.at[0]),
        pltpu.make_async_copy(gain, g_v, small_sem.at[1]),
    )
    for copy in small:
        copy.start()
    for i in range(blocks):
        for copy in load(i):
            copy.start()

    barrier = pltpu.get_barrier_semaphore()

    def signal(sem, peer):
        pl.semaphore_signal(sem, inc=1, device_id=peer, device_id_type=MESH)

    for k in range(1, zero):
        peer = lax.rem(y + k, zero)

        @pl.when(peer != 0)
        def _(peer=peer):
            signal(barrier, {"zero": peer})

    others = [at_core(1)]
    others += [at_x(k) for k in range(1, X)]
    others += [at_z(k) for k in range(1, depth)]

    for copy in small:
        copy.wait()
    part[...] = (w_v[...] * g_v[...]).astype(jnp.bfloat16).astype(jnp.float32)

    for i in range(blocks):
        at = pl.ds(i * BLOCK, BLOCK)
        for copy in load(i):
            copy.wait()
        value = merged[at] + added[at].astype(jnp.float32)
        merged[at] = value
        square = value * value
        lanes = square[:, :128]
        for j in range(128, cols, 128):
            lanes = lanes + square[:, j : j + 128]
        own_sum[:, at] = jnp.sum(lanes.T, axis=0, keepdims=True)
    sums[y] = own_sum[...]

    @pl.when(y != 0)
    def _():
        pl.semaphore_wait(barrier, zero - 1)

    @pl.when(y == 1)
    def _():
        signal(ready, {"zero": 0})

    @pl.when(y == 0)
    def _():
        pl.semaphore_wait(ready, 1)

    def send_sum(k):
        return pltpu.make_async_remote_copy(
            own_sum, sums.at[y], sum_send.at[k - 1], sum_recv.at[k - 1],
            device_id={"zero": lax.rem(y + k, zero)}, device_id_type=MESH,
        )

    def send_part(k):
        return pltpu.make_async_remote_copy(
            part, column.at[y], part_send.at[k - 1], part_recv.at[k - 1],
            device_id={"zero": lax.rem(y + k, zero)}, device_id_type=MESH,
        )

    def send_early(way):
        peer = lax.rem(y + (1 if way == 0 else zero - 1), zero)
        return pltpu.make_async_remote_copy(
            merged.at[pl.ds(0, EARLY * CHUNK)], early.at[way], early_send.at[way], early_recv.at[way],
            device_id={"zero": peer}, device_id_type=MESH,
        )

    for k in (4, 3, 5, 2, 6, 1, 7):
        send_sum(k).start()
    for way in (0, 1):
        send_early(way).start()
    for k in range(1, zero):
        send_part(k).start()

    @pl.when(y == 0)
    def _():
        for peer in others:
            signal(barrier, {"bank": peer})

    own_part = pltpu.make_async_copy(part, column.at[y], local_sem.at[0])
    own_part.start()

    for k in range(1, zero):
        send_sum(k).wait_recv()
    total = jnp.sqrt(jnp.sum(sums[...], axis=0))
    scale[...] = total
    own_sum_inverse = 1.0 / total
    for i in range(blocks):
        at = slice(i * BLOCK, (i + 1) * BLOCK)
        inverse[at] = jnp.broadcast_to(own_sum_inverse[:, at], (BLOCK, BLOCK)).T

    def ring(way, hop, c):
        step = 1 if way == 0 else zero - 1
        owner = lax.rem(y + (zero - step) * hop, zero)
        at = final.at[pl.ds(c * CHUNK, CHUNK), pl.ds(pl.multiple_of(owner * cols, cols), cols)]
        return pltpu.make_async_remote_copy(
            at, at, ring_send.at[way, hop, c], ring_recv.at[way, hop, c],
            device_id={"zero": lax.rem(y + step, zero)}, device_id_type=MESH,
        )

    def narrow(source, c, owner):
        at = pl.ds(pl.multiple_of(c * CHUNK, CHUNK), CHUNK)
        wide = jnp.concatenate([inverse[at]] * (cols // 128), axis=1)
        final[at, pl.ds(pl.multiple_of(owner * cols, cols), cols)] = (source[at] * wide).astype(jnp.bfloat16)

    def own(c, _):
        narrow(merged, c, y)

        @pl.when(c > EARLY)
        def _():
            ring(0, 0, c - 1).start()
            ring(1, 0, c - 1).start()

        return 0

    lax.fori_loop(EARLY, chunks, own, 0)

    def own_early(c, _):
        narrow(merged, c, y)
        return 0

    lax.fori_loop(0, EARLY, own_early, 0)
    ring(0, 0, chunks - 1).start()
    ring(1, 0, chunks - 1).start()

    for way in (0, 1):
        send_early(way).wait_recv()
    left, right = lax.rem(y + zero - 1, zero), lax.rem(y + 1, zero)

    def neighbours_early(c, _):
        narrow(early.at[0], c, left)
        narrow(early.at[1], c, right)

        @pl.when(c > 0)
        def _():
            ring(0, 1, c - 1).start()
            ring(1, 1, c - 1).start()

        return 0

    lax.fori_loop(0, EARLY, neighbours_early, 0)

    @pl.when(y == 0)
    def _():
        pl.semaphore_wait(barrier, len(others))
        for k in range(1, zero):
            signal(opened, {"zero": k})

    @pl.when(y != 0)
    def _():
        pl.semaphore_wait(opened, 1)

    own_part.wait()
    for k in range(1, zero):
        send_part(k).wait_recv()

    def send_table(sem, rows_at, count, peer):
        at = table.at[pl.ds(rows_at, count)]
        return pltpu.make_async_remote_copy(
            at, at, table_send.at[sem], table_recv.at[sem],
            device_id={"bank": peer}, device_id_type=MESH,
        )

    own_row = pltpu.make_async_copy(column, table.at[bank], local_sem.at[1])
    own_row.start()
    own_row.wait()
    stages = [
        [send_table(0, bank, 1, at_core(1))],
        [send_table(k, bank - core, CORES, at_x(k)) for k in range(1, X)],
        [send_table(X - 1 + k, chip_z * X * CORES, X * CORES, at_z(k)) for k in range(1, depth)],
    ]

    def table_stage(s):
        if s:
            for copy in stages[s - 1]:
                copy.wait_recv()
        if s < len(stages):
            for copy in stages[s]:
                copy.start()
        else:
            width = part.shape[1]
            for j in range(zero):
                router[:, j * width : (j + 1) * width] = table[:, j, 0, :].astype(jnp.bfloat16)

    def relay(hop, ways, first, last):
        def step(c, _):
            for way in (0, 1):
                ring(way, hop - 1, c).wait_recv()
                if way in ways:
                    ring(way, hop, c).start()
            return 0

        lax.fori_loop(first, last, step, 0)

    ring(0, 1, EARLY - 1).start()
    ring(1, 1, EARLY - 1).start()
    table_stage(0)
    relay(1, (0, 1), EARLY, half)
    table_stage(1)
    relay(1, (0, 1), half, chunks)
    table_stage(2)
    relay(2, (0, 1), 0, chunks)
    table_stage(3)
    relay(3, (0,), 0, half)
    relay(3, (1,), half, chunks)

    def last_cw(c, _):
        ring(0, 3, c).wait_recv()
        ring(1, 3, c + half).wait_recv()
        return 0

    lax.fori_loop(0, half, last_cw, 0)

    def sent_first(c, _):
        for way in (0, 1):
            ring(way, 0, c).wait_send()
        return 0

    def sent(c, _):
        for hop in (1, 2):
            for way in (0, 1):
                ring(way, hop, c).wait_send()
        return 0

    for way in (0, 1):
        send_early(way).wait_send()
    lax.fori_loop(EARLY, chunks, sent_first, 0)
    lax.fori_loop(0, chunks, sent, 0)

    def sent_last(c, _):
        ring(0, 3, c).wait_send()
        ring(1, 3, c + half).wait_send()
        return 0

    lax.fori_loop(0, half, sent_last, 0)
    for k in range(1, zero):
        send_sum(k).wait_send()
        send_part(k).wait_send()
    for stage in stages:
        for copy in stage:
            copy.wait_send()


def write(final, scale, router, final_out, scale_out, router_out, sem):
    copies = [
        pltpu.make_async_copy(scale, scale_out, sem.at[0]),
        pltpu.make_async_copy(router, router_out, sem.at[1]),
    ]
    for i in range(final.shape[0] // BLOCK):
        at = pl.ds(i * BLOCK, BLOCK)
        copies.append(pltpu.make_async_copy(final.at[at], final_out.at[at], sem.at[2 + i]))
    for copy in copies:
        copy.start()
    for copy in copies:
        copy.wait()


def in_hbm(value):
    return pltpu.with_memory_space_constraint(value, pltpu.HBM)


def body(master_down, second_down, router_weight, router_gain):
    _, rows, cols = master_down.shape
    width = router_weight.shape[0]
    zero, banks = lax.axis_size("zero"), lax.axis_size("bank")
    blocks, chunks = rows // BLOCK, rows // CHUNK
    depth = banks // (X * CORES)
    f32, vmem, dma = jnp.float32, pltpu.VMEM, pltpu.SemaphoreType.DMA
    final, scale, router = pl.pallas_call(
        kernel,
        out_shape=(
            jax.ShapeDtypeStruct((rows, zero * cols), jnp.bfloat16),
            jax.ShapeDtypeStruct((1, rows), f32),
            jax.ShapeDtypeStruct((banks, zero * width), jnp.bfloat16),
        ),
        in_specs=[pl.BlockSpec(memory_space=pltpu.HBM)] * 4,
        out_specs=[pl.BlockSpec(memory_space=vmem)] * 3,
        scratch_shapes=[
            vmem((rows, cols), f32),
            vmem((rows, cols), jnp.bfloat16),
            vmem((rows, 128), f32),
            vmem((1, rows), f32),
            vmem((zero, 1, rows), f32),
            vmem((1, width), f32),
            vmem((1, width), f32),
            vmem((1, width), f32),
            vmem((zero, 1, width), f32),
            vmem((banks, zero, 1, width), f32),
            vmem((2, EARLY * CHUNK, cols), f32),
            pltpu.SemaphoreType.REGULAR,
            pltpu.SemaphoreType.REGULAR,
            dma((2,)),
            dma((2,)),
            dma((2, blocks)),
            dma((2,)),
            dma((2,)),
            dma((zero - 1,)),
            dma((zero - 1,)),
            dma((2, 4, chunks)),
            dma((2, 4, chunks)),
            dma((zero - 1,)),
            dma((zero - 1,)),
            dma((X - 1 + depth,)),
            dma((X - 1 + depth,)),
        ],
        compiler_params=pltpu.CompilerParams(
            collective_id=0, has_side_effects=True, vmem_limit_bytes=40 * 2**20
        ),
        name="gather",
    )(
        in_hbm(master_down.reshape(rows, cols)),
        in_hbm(second_down.reshape(rows, cols)),
        in_hbm(router_weight.reshape(1, width)),
        in_hbm(router_gain.reshape(1, width)),
    )
    final, scale, router = pl.pallas_call(
        write,
        out_shape=tuple(jax.ShapeDtypeStruct(x.shape, x.dtype) for x in (final, scale, router)),
        in_specs=[pl.BlockSpec(memory_space=pl.ANY)] * 3,
        out_specs=[pl.BlockSpec(memory_space=pl.ANY)] * 3,
        scratch_shapes=[dma((blocks + 2,))],
        compiler_params=pltpu.CompilerParams(vmem_limit_bytes=2**20),
        name="write",
    )(*(pltpu.with_memory_space_constraint(x, vmem) for x in (final, scale, router)))
    return final.reshape(1, rows, zero * cols), scale, router.T


def solution(mesh):
    return jax.shard_map(
        body,
        mesh=mesh,
        in_specs=(P("bank", None, "zero"), P("bank", None, "zero"), P("zero", "bank"), P("zero")),
        out_specs=(P("bank", None, None), P("bank", None), P()),
        check_vma=False,
    )
```

```python
import jax
import jax.numpy as jnp
from jax import lax
from jax.experimental import pallas as pl
from jax.experimental.pallas import tpu as pltpu
from jax.sharding import PartitionSpec as P

MESH = pl.DeviceIdType.MESH
BLOCK = 128
CHUNKS = 4
LOADS = 4
EARLY = 0
X, CORES = 4, 2


def kernel(
    master, second, weight, gain,
    final, scale, router,
    merged, added, own_sum, sums, w_v, g_v, part, column, table, early,
    ready, opened, load_sem, small_sem, local_sem,
    sum_send, sum_recv, part_send, part_recv, table_send, table_recv,
    early_send, early_recv, own_send, relay_send, ring_recv,
):
    rows, cols = merged.shape
    zero = lax.axis_size("zero")
    blocks, chunk, half = rows // BLOCK, rows // CHUNKS, CHUNKS // 2
    y, bank = lax.axis_index("zero"), lax.axis_index("bank")
    chip_z, chip_x = bank // (X * CORES), lax.rem(bank // CORES, X)
    depth = lax.axis_size("bank") // (X * CORES)
    core = lax.rem(bank, CORES)

    def at_core(k):
        return bank - core + lax.rem(core + k, CORES)

    def at_x(k):
        return (chip_z * X + lax.rem(chip_x + k, X)) * CORES + core

    def at_z(k):
        return (lax.rem(chip_z + k, depth) * X + chip_x) * CORES + core

    def signal(sem, peer):
        pl.semaphore_signal(sem, inc=1, device_id=peer, device_id_type=MESH)

    def arrived(ref, sem):
        pltpu.make_async_copy(ref, ref, sem).wait()

    def remote(source, target, send_sem, recv_sem, peer):
        return pltpu.make_async_remote_copy(
            source, target, send_sem, recv_sem, device_id=peer, device_id_type=MESH
        )

    barrier = pltpu.get_barrier_semaphore()
    for k in range(1, zero):
        peer = lax.rem(y + k, zero)

        @pl.when(peer != 0)
        def _(peer=peer):
            signal(barrier, {"zero": peer})

    step = rows // LOADS
    for i in range(LOADS):
        at = pl.ds(i * step, step)
        pltpu.make_async_copy(master.at[at], merged.at[at], load_sem.at[0]).start()
        pltpu.make_async_copy(second.at[at], added.at[at], load_sem.at[1]).start()
    small = (
        pltpu.make_async_copy(weight, w_v, small_sem.at[0]),
        pltpu.make_async_copy(gain, g_v, small_sem.at[1]),
    )
    for copy in small:
        copy.start()

    arrived(merged, load_sem.at[0])
    arrived(added, load_sem.at[1])
    for i in range(blocks):
        at = pl.ds(i * BLOCK, BLOCK)
        value = merged[at] + added[at].astype(jnp.float32)
        merged[at] = value
        square = value * value
        lanes = square[:, :128]
        for j in range(128, cols, 128):
            lanes = lanes + square[:, j : j + 128]
        own_sum[:, at] = jnp.sum(lanes.T, axis=0, keepdims=True)
    sums[y] = own_sum[...]

    for copy in small:
        copy.wait()
    part[...] = (w_v[...] * g_v[...]).astype(jnp.bfloat16).astype(jnp.float32)

    @pl.when(y != 0)
    def _():
        pl.semaphore_wait(barrier, zero - 1)

    @pl.when(y == 1)
    def _():
        signal(ready, {"zero": 0})

    @pl.when(y == 0)
    def _():
        pl.semaphore_wait(ready, 1)

    left, right = lax.rem(y + zero - 1, zero), lax.rem(y + 1, zero)

    def early_rows(way):
        return pl.ds(0 if way == 0 else rows - EARLY * BLOCK, EARLY * BLOCK)

    def send_early(way):
        return remote(
            merged.at[early_rows(way)], early.at[way], early_send.at[way], early_recv.at[way],
            {"zero": right if way == 0 else left},
        )

    for k in (4, 3, 5, 2, 6, 1, 7):
        remote(own_sum, sums.at[y], sum_send, sum_recv, {"zero": lax.rem(y + k, zero)}).start()
    if EARLY:
        for way in (0, 1):
            send_early(way).start()
    for k in range(1, zero):
        remote(part, column.at[y], part_send, part_recv, {"zero": lax.rem(y + k, zero)}).start()
    own_part = pltpu.make_async_copy(part, column.at[y], local_sem)
    own_part.start()

    others = [at_core(1)]
    others += [at_x(k) for k in range(1, X)]
    others += [at_z(k) for k in range(1, depth)]

    @pl.when(y == 0)
    def _():
        for peer in others:
            signal(barrier, {"bank": peer})

    arrived(sums.at[pl.ds(0, zero - 1)], sum_recv)
    total = jnp.sqrt(jnp.sum(sums[...], axis=0))
    scale[...] = total
    inverse = 1.0 / total

    def columns(owner):
        return pl.ds(pl.multiple_of(owner * cols, cols), cols)

    def narrow(source, block, owner):
        at = slice(block * BLOCK, (block + 1) * BLOCK)
        tall = jnp.broadcast_to(inverse[:, at], (BLOCK, BLOCK)).T
        wide = jnp.concatenate([tall] * (cols // 128), axis=1)
        final[at, columns(owner)] = (source[...] * wide).astype(jnp.bfloat16)

    def ring(way, hop, place):
        c = place if way == 0 else CHUNKS - 1 - place
        start, count = c * chunk, chunk
        if hop == 0 and place == 0:
            start, count = start + (EARLY * BLOCK if way == 0 else 0), count - EARLY * BLOCK
        owner = lax.rem(y + (zero - hop if way == 0 else hop), zero)
        at = final.at[pl.ds(start, count), columns(owner)]
        sem = own_send if hop == 0 else relay_send
        return remote(
            at, at, sem.at[way], ring_recv.at[way, hop * CHUNKS + place],
            {"zero": right if way == 0 else left},
        )

    mine = list(range(EARLY, blocks - EARLY))
    order = []
    for place in range(CHUNKS):
        for way in (0, 1):
            c = place if way == 0 else CHUNKS - 1 - place
            need = [i for i in mine if i * BLOCK < (c + 1) * chunk and (i + 1) * BLOCK > c * chunk]
            order.append(([i for i in need if all(i not in o[0] for o in order)], way, place))
    waiting = None
    for need, way, place in order:
        for i in need:
            narrow(merged.at[pl.ds(i * BLOCK, BLOCK)], i, y)
        if waiting and need:
            ring(*waiting).start()
            waiting = None
        elif waiting:
            ring(*waiting).start()
        waiting = (way, 0, place)
    for i in range(blocks):
        if i not in mine:
            narrow(merged.at[pl.ds(i * BLOCK, BLOCK)], i, y)
    ring(*waiting).start()

    if EARLY:
        for way in (0, 1):
            send_early(way).wait_recv()
            for i in range(EARLY):
                first = early_rows(way).start // BLOCK
                narrow(early.at[way, pl.ds(i * BLOCK, BLOCK)], first + i, left if way == 0 else right)

    @pl.when(y == 0)
    def _():
        pl.semaphore_wait(barrier, len(others))
        for k in range(1, zero):
            signal(opened, {"zero": k})

    @pl.when(y != 0)
    def _():
        pl.semaphore_wait(opened, 1)

    own_part.wait()
    arrived(column.at[pl.ds(0, zero - 1)], part_recv)
    own_row = pltpu.make_async_copy(column, table.at[bank], local_sem)
    own_row.start()
    own_row.wait()
    stages = [
        (bank, 1, [at_core(1)]),
        (bank - core, CORES, [at_x(k) for k in range(1, X)]),
        (chip_z * X * CORES, X * CORES, [at_z(k) for k in range(1, depth)]),
    ]

    def table_stage(s):
        if s:
            _, count, peers = stages[s - 1]
            arrived(table.at[pl.ds(0, count * len(peers))], table_recv.at[s - 1])
        if s < len(stages):
            first, count, peers = stages[s]
            at = table.at[pl.ds(first, count)]
            for peer in peers:
                remote(at, at, table_send, table_recv.at[s], {"bank": peer}).start()
        else:
            width = part.shape[1]
            for j in range(zero):
                router[:, j * width : (j + 1) * width] = table[:, j, 0, :].astype(jnp.bfloat16)

    for hop in (1, 2, 3, 4):
        for place in range(CHUNKS if hop < 4 else half):
            for way in (0, 1):
                ring(way, hop - 1, place).wait_recv()
                if hop < 3 or (hop == 3 and place < half):
                    ring(way, hop, place).start()
            if hop == 1:
                table_stage(place)

    for way in (0, 1):
        arrived(final.at[pl.ds(0, rows - EARLY * BLOCK), pl.ds(0, cols)], own_send.at[way])
        arrived(final.at[pl.ds(0, rows // 2), pl.ds(0, 5 * cols)], relay_send.at[way])
        if EARLY:
            send_early(way).wait_send()
    arrived(sums.at[pl.ds(0, zero - 1)], sum_send)
    arrived(column.at[pl.ds(0, zero - 1)], part_send)
    arrived(table.at[pl.ds(0, table.shape[0] - 1)], table_send)


def write(final, scale, router, final_out, scale_out, router_out, sem):
    copies = [
        pltpu.make_async_copy(final, final_out, sem.at[0]),
        pltpu.make_async_copy(router, router_out, sem.at[1]),
        pltpu.make_async_copy(scale, scale_out, sem.at[2]),
    ]
    for copy in copies:
        copy.start()
    for copy in copies:
        copy.wait()


def body(master_down, second_down, router_weight, router_gain):
    _, rows, cols = master_down.shape
    width = router_weight.shape[0]
    zero, banks = lax.axis_size("zero"), lax.axis_size("bank")
    f32, vmem, dma = jnp.float32, pltpu.VMEM, pltpu.SemaphoreType.DMA
    args = (
        master_down.reshape(rows, cols),
        second_down.reshape(rows, cols),
        router_weight.reshape(1, width),
        router_gain.reshape(1, width),
    )
    results = pl.pallas_call(
        kernel,
        out_shape=(
            jax.ShapeDtypeStruct((rows, zero * cols), jnp.bfloat16),
            jax.ShapeDtypeStruct((1, rows), f32),
            jax.ShapeDtypeStruct((banks, zero * width), jnp.bfloat16),
        ),
        in_specs=[pl.BlockSpec(memory_space=pltpu.HBM)] * 4,
        out_specs=[pl.BlockSpec(memory_space=vmem)] * 3,
        scratch_shapes=[
            vmem((rows, cols), f32),
            vmem((rows, cols), jnp.bfloat16),
            vmem((1, rows), f32),
            vmem((zero, 1, rows), f32),
            vmem((1, width), f32),
            vmem((1, width), f32),
            vmem((1, width), f32),
            vmem((zero, 1, width), f32),
            vmem((banks, zero, 1, width), f32),
            vmem((2, max(EARLY, 1) * BLOCK, cols), f32),
            pltpu.SemaphoreType.REGULAR,
            pltpu.SemaphoreType.REGULAR,
            dma((2,)),
            dma((2,)),
            dma(()),
            dma(()),
            dma(()),
            dma(()),
            dma(()),
            dma(()),
            dma((3,)),
            dma((2,)),
            dma((2,)),
            dma((2,)),
            dma((2,)),
            dma((2, 7 * CHUNKS // 2)),
        ],
        compiler_params=pltpu.CompilerParams(
            collective_id=0, has_side_effects=True, vmem_limit_bytes=40 * 2**20
        ),
        name="gather",
    )(*map(in_hbm, args))
    final, scale, router = pl.pallas_call(
        write,
        out_shape=tuple(jax.ShapeDtypeStruct(x.shape, x.dtype) for x in results),
        in_specs=[pl.BlockSpec(memory_space=pl.ANY)] * 3,
        out_specs=[pl.BlockSpec(memory_space=pl.ANY)] * 3,
        scratch_shapes=[dma((3,))],
        compiler_params=pltpu.CompilerParams(vmem_limit_bytes=2**20),
        name="write",
    )(*(pltpu.with_memory_space_constraint(x, vmem) for x in results))
    return final.reshape(1, rows, zero * cols), scale, router.T


def in_hbm(value):
    return pltpu.with_memory_space_constraint(value, pltpu.HBM)


def solution(mesh):
    return jax.shard_map(
        body,
        mesh=mesh,
        in_specs=(P("bank", None, "zero"), P("bank", None, "zero"), P("zero", "bank"), P("zero")),
        out_specs=(P("bank", None, None), P("bank", None), P()),
        check_vma=False,
    )
```

```python
import jax
import jax.numpy as jnp
from jax import lax
from jax.experimental import pallas as pl
from jax.experimental.pallas import tpu as pltpu
from jax.sharding import PartitionSpec as P

MESH = pl.DeviceIdType.MESH
BLOCK = 128
HALVES = 2
FIRST = 352
LOADS = 4
EARLY = 128
X, CORES = 4, 2


def kernel(
    master, second, weight, gain,
    final, scale, router,
    merged, added, own_sum, sums, w_v, g_v, part, column, table, early,
    ready, opened, load_sem, small_sem, local_sem,
    sum_send, sum_recv, part_send, part_recv, table_send, table_recv,
    early_send, early_recv, own_send, relay_send, ring_recv,
):
    rows, cols = merged.shape
    zero = lax.axis_size("zero")
    blocks, half = rows // BLOCK, rows // HALVES
    y, bank = lax.axis_index("zero"), lax.axis_index("bank")
    chip_z, chip_x = bank // (X * CORES), lax.rem(bank // CORES, X)
    depth = lax.axis_size("bank") // (X * CORES)
    core = lax.rem(bank, CORES)

    def at_core(k):
        return bank - core + lax.rem(core + k, CORES)

    def at_x(k):
        return (chip_z * X + lax.rem(chip_x + k, X)) * CORES + core

    def at_z(k):
        return (lax.rem(chip_z + k, depth) * X + chip_x) * CORES + core

    def signal(sem, peer):
        pl.semaphore_signal(sem, inc=1, device_id=peer, device_id_type=MESH)

    def arrived(ref, sem):
        pltpu.make_async_copy(ref, ref, sem).wait()

    def remote(source, target, send_sem, recv_sem, peer):
        return pltpu.make_async_remote_copy(
            source, target, send_sem, recv_sem, device_id=peer, device_id_type=MESH
        )

    barrier = pltpu.get_barrier_semaphore()
    for k in range(1, zero):
        peer = lax.rem(y + k, zero)

        @pl.when(peer != 0)
        def _(peer=peer):
            signal(barrier, {"zero": peer})

    step = rows // LOADS
    for i in range(LOADS):
        at = pl.ds(i * step, step)
        pltpu.make_async_copy(master.at[at], merged.at[at], load_sem.at[0]).start()
        pltpu.make_async_copy(second.at[at], added.at[at], load_sem.at[1]).start()
    small = (
        pltpu.make_async_copy(weight, w_v, small_sem.at[0]),
        pltpu.make_async_copy(gain, g_v, small_sem.at[1]),
    )
    for copy in small:
        copy.start()

    arrived(merged, load_sem.at[0])
    arrived(added, load_sem.at[1])
    for i in range(blocks):
        at = pl.ds(i * BLOCK, BLOCK)
        value = merged[at] + added[at].astype(jnp.float32)
        merged[at] = value
        square = value * value
        lanes = square[:, :128]
        for j in range(128, cols, 128):
            lanes = lanes + square[:, j : j + 128]
        own_sum[:, at] = jnp.sum(lanes.T, axis=0, keepdims=True)
    sums[y] = own_sum[...]

    for copy in small:
        copy.wait()
    part[...] = (w_v[...] * g_v[...]).astype(jnp.bfloat16).astype(jnp.float32)

    @pl.when(y != 0)
    def _():
        pl.semaphore_wait(barrier, zero - 1)

    @pl.when(y == zero - 1)
    def _():
        signal(ready, {"zero": 0})

    @pl.when(y == 0)
    def _():
        pl.semaphore_wait(ready, 1)

    left, right = lax.rem(y + zero - 1, zero), lax.rem(y + 1, zero)

    def early_rows(way):
        return pl.ds(0 if way == 0 else rows - EARLY, EARLY)

    def send_early(way):
        return remote(
            merged.at[early_rows(way)], early.at[way], early_send.at[way], early_recv.at[way],
            {"zero": right if way == 0 else left},
        )

    for k in (4, 3, 5, 2, 6, 1, 7):
        remote(own_sum, sums.at[y], sum_send, sum_recv, {"zero": lax.rem(y + k, zero)}).start()
    if EARLY:
        for way in (0, 1):
            send_early(way).start()
    for k in range(1, zero):
        remote(part, column.at[y], part_send, part_recv, {"zero": lax.rem(y + k, zero)}).start()
    own_part = pltpu.make_async_copy(part, column.at[y], local_sem)
    own_part.start()

    others = [at_core(1)]
    others += [at_x(k) for k in range(1, X)]
    others += [at_z(k) for k in range(1, depth)]

    @pl.when(y == 0)
    def _():
        for peer in others:
            signal(barrier, {"bank": peer})

    arrived(sums.at[pl.ds(0, zero - 1)], sum_recv)
    total = jnp.sqrt(jnp.sum(sums[...], axis=0))
    scale[...] = total
    inverse = 1.0 / total

    def columns(owner):
        return pl.ds(pl.multiple_of(owner * cols, cols), cols)

    def narrow(source, start, count, owner):
        block = start // BLOCK * BLOCK
        tall = jnp.broadcast_to(inverse[:, block : block + BLOCK], (BLOCK, BLOCK)).T
        wide = jnp.concatenate([tall[start - block : start - block + count]] * (cols // 128), axis=1)
        final[start : start + count, columns(owner)] = (source[...] * wide).astype(jnp.bfloat16)

    def ring(way, hop, place, first=0, last=half):
        if way == 0:
            start = place * half + first
        else:
            start = rows - place * half - last
        owner = lax.rem(y + (zero - hop if way == 0 else hop), zero)
        at = final.at[pl.ds(start, last - first), columns(owner)]
        sem = own_send if hop == 0 else relay_send
        return remote(
            at, at, sem.at[way], ring_recv.at[way, hop * HALVES + place],
            {"zero": right if way == 0 else left},
        )

    done, waiting = set(), None

    def own(start, stop):
        for i in range(start // BLOCK, -(-stop // BLOCK)):
            if i not in done:
                done.add(i)
                narrow(merged.at[pl.ds(i * BLOCK, BLOCK)], i * BLOCK, BLOCK, y)

    for place, first, last in ((0, EARLY, FIRST), (0, FIRST, half), (1, 0, FIRST), (1, FIRST, half)):
        for way in (0, 1):
            start, stop = place * half + first, place * half + last
            own(*((start, stop) if way == 0 else (rows - stop, rows - start)))
            if waiting:
                ring(*waiting).start()
            waiting = (way, 0, place, first, last)
    own(0, rows)

    if EARLY:
        for way in (0, 1):
            send_early(way).wait_recv()
            first = early_rows(way).start
            for start in range(first, first + EARLY, 64):
                narrow(early.at[way, pl.ds(start - first, 64)], start, 64, left if way == 0 else right)
    ring(*waiting).start()

    stages = [
        (bank, 1, [at_core(1)]),
        (bank - core, CORES, [at_x(k) for k in range(1, X)]),
        (chip_z * X * CORES, X * CORES, [at_z(k) for k in range(1, depth)]),
    ]

    def table_stage(s):
        if s:
            _, count, peers = stages[s - 1]
            arrived(table.at[pl.ds(0, count * len(peers))], table_recv.at[s - 1])
        else:
            own_part.wait()
            arrived(column.at[pl.ds(0, zero - 1)], part_recv)
            own_row = pltpu.make_async_copy(column, table.at[bank], local_sem)
            own_row.start()
            own_row.wait()
        if s < len(stages):
            first, count, peers = stages[s]
            at = table.at[pl.ds(first, count)]
            for peer in peers:
                remote(at, at, table_send, table_recv.at[s], {"bank": peer}).start()
        else:
            width = part.shape[1]
            for j in range(zero):
                router[:, j * width : (j + 1) * width] = table[:, j, 0, :].astype(jnp.bfloat16)

    def open_gate():
        @pl.when(y == 0)
        def _():
            pl.semaphore_wait(barrier, len(others))
            for k in range(1, zero):
                signal(opened, {"zero": k})

    def pass_gate():
        @pl.when(y != 0)
        def _():
            pl.semaphore_wait(opened, 1)

        table_stage(0)

    between = {
        (1, 0): open_gate,
        (1, 1): pass_gate,
        (2, 0): lambda: table_stage(1),
        (2, 1): lambda: table_stage(2),
        (3, 0): lambda: table_stage(3),
    }
    for hop in (1, 2, 3, 4):
        for place in range(HALVES if hop < 4 else 1):
            for way in (0, 1):
                arrival = ring(way, hop - 1, place, EARLY if (hop, place) == (1, 0) else 0)
                arrival.wait_recv()
                if hop < 3 or (hop == 3 and place == 0):
                    ring(way, hop, place).start()
            if (hop, place) in between:
                between[hop, place]()

    for way in (0, 1):
        arrived(final.at[pl.ds(0, rows - EARLY), pl.ds(0, cols)], own_send.at[way])
        arrived(final.at[pl.ds(0, rows // 2), pl.ds(0, 5 * cols)], relay_send.at[way])
        if EARLY:
            send_early(way).wait_send()
    arrived(sums.at[pl.ds(0, zero - 1)], sum_send)
    arrived(column.at[pl.ds(0, zero - 1)], part_send)
    arrived(table.at[pl.ds(0, table.shape[0] - 1)], table_send)


def write(final, scale, router, final_out, scale_out, router_out, sem):
    copies = [
        pltpu.make_async_copy(final, final_out, sem.at[0]),
        pltpu.make_async_copy(router, router_out, sem.at[1]),
        pltpu.make_async_copy(scale, scale_out, sem.at[2]),
    ]
    for copy in copies:
        copy.start()
    for copy in copies:
        copy.wait()


def body(master_down, second_down, router_weight, router_gain):
    _, rows, cols = master_down.shape
    width = router_weight.shape[0]
    zero, banks = lax.axis_size("zero"), lax.axis_size("bank")
    f32, vmem, dma = jnp.float32, pltpu.VMEM, pltpu.SemaphoreType.DMA
    args = (
        master_down.reshape(rows, cols),
        second_down.reshape(rows, cols),
        router_weight.reshape(1, width),
        router_gain.reshape(1, width),
    )
    results = pl.pallas_call(
        kernel,
        out_shape=(
            jax.ShapeDtypeStruct((rows, zero * cols), jnp.bfloat16),
            jax.ShapeDtypeStruct((1, rows), f32),
            jax.ShapeDtypeStruct((banks, zero * width), jnp.bfloat16),
        ),
        in_specs=[pl.BlockSpec(memory_space=pltpu.HBM)] * 4,
        out_specs=[pl.BlockSpec(memory_space=vmem)] * 3,
        scratch_shapes=[
            vmem((rows, cols), f32),
            vmem((rows, cols), jnp.bfloat16),
            vmem((1, rows), f32),
            vmem((zero, 1, rows), f32),
            vmem((1, width), f32),
            vmem((1, width), f32),
            vmem((1, width), f32),
            vmem((zero, 1, width), f32),
            vmem((banks, zero, 1, width), f32),
            vmem((2, max(EARLY, 8), cols), f32),
            pltpu.SemaphoreType.REGULAR,
            pltpu.SemaphoreType.REGULAR,
            dma((2,)),
            dma((2,)),
            dma(()),
            dma(()),
            dma(()),
            dma(()),
            dma(()),
            dma(()),
            dma((3,)),
            dma((2,)),
            dma((2,)),
            dma((2,)),
            dma((2,)),
            dma((2, 3 * HALVES + 1)),
        ],
        compiler_params=pltpu.CompilerParams(
            collective_id=0, has_side_effects=True, vmem_limit_bytes=40 * 2**20
        ),
        name="gather",
    )(*map(in_hbm, args))
    final, scale, router = pl.pallas_call(
        write,
        out_shape=tuple(jax.ShapeDtypeStruct(x.shape, x.dtype) for x in results),
        in_specs=[pl.BlockSpec(memory_space=pl.ANY)] * 3,
        out_specs=[pl.BlockSpec(memory_space=pl.ANY)] * 3,
        scratch_shapes=[dma((3,))],
        compiler_params=pltpu.CompilerParams(vmem_limit_bytes=2**20),
        name="write",
    )(*(pltpu.with_memory_space_constraint(x, vmem) for x in results))
    return final.reshape(1, rows, zero * cols), scale, router.T


def in_hbm(value):
    return pltpu.with_memory_space_constraint(value, pltpu.HBM)


def solution(mesh):
    return jax.shard_map(
        body,
        mesh=mesh,
        in_specs=(P("bank", None, "zero"), P("bank", None, "zero"), P("zero", "bank"), P("zero")),
        out_specs=(P("bank", None, None), P("bank", None), P()),
        check_vma=False,
    )
```

```python
import jax
import jax.numpy as jnp
from jax import lax
from jax.experimental import pallas as pl
from jax.experimental.pallas import tpu as pltpu
from jax.sharding import PartitionSpec as P

MESH = pl.DeviceIdType.MESH
BLOCK = 128
HALVES = 2
FIRST = 352
LOADS = 4
EARLY = 128
LEAST = 0
GATE, HERALD = 7, 6
X, CORES = 4, 2


def kernel(
    master, second, weight, gain,
    final, scale, router,
    merged, added, own_sum, sums, w_v, g_v, part, column, table, early,
    ready, opened, load_sem, small_sem, local_sem,
    sum_send, sum_recv, part_send, part_recv, table_send, table_recv,
    early_send, early_recv, ring_send, ring_recv,
):
    rows, cols = merged.shape
    zero = lax.axis_size("zero")
    blocks, half = rows // BLOCK, rows // HALVES
    y, bank = lax.axis_index("zero"), lax.axis_index("bank")
    chip_z, chip_x = bank // (X * CORES), lax.rem(bank // CORES, X)
    depth = lax.axis_size("bank") // (X * CORES)
    core = lax.rem(bank, CORES)

    def at_core(k):
        return bank - core + lax.rem(core + k, CORES)

    def at_x(k):
        return (chip_z * X + lax.rem(chip_x + k, X)) * CORES + core

    def at_z(k):
        return (lax.rem(chip_z + k, depth) * X + chip_x) * CORES + core

    def signal(sem, peer):
        pl.semaphore_signal(sem, inc=1, device_id=peer, device_id_type=MESH)

    def arrived(ref, sem):
        pltpu.make_async_copy(ref, ref, sem).wait()

    def remote(source, target, send_sem, recv_sem, peer):
        return pltpu.make_async_remote_copy(
            source, target, send_sem, recv_sem, device_id=peer, device_id_type=MESH
        )

    barrier = pltpu.get_barrier_semaphore()
    for k in range(1, zero):
        peer = lax.rem(y + k, zero)

        @pl.when(peer != GATE)
        def _(peer=peer):
            signal(barrier, {"zero": peer})

    step = rows // LOADS
    for i in range(LOADS):
        at = pl.ds(i * step, step)
        pltpu.make_async_copy(master.at[at], merged.at[at], load_sem.at[0]).start()
        pltpu.make_async_copy(second.at[at], added.at[at], load_sem.at[1]).start()
    small = (
        pltpu.make_async_copy(weight, w_v, small_sem.at[0]),
        pltpu.make_async_copy(gain, g_v, small_sem.at[1]),
    )
    for copy in small:
        copy.start()

    arrived(merged, load_sem.at[0])
    arrived(added, load_sem.at[1])
    for i in range(blocks):
        at = pl.ds(i * BLOCK, BLOCK)
        value = merged[at] + added[at].astype(jnp.float32)
        merged[at] = value
        square = value * value
        lanes = square[:, :128]
        for j in range(128, cols, 128):
            lanes = lanes + square[:, j : j + 128]
        own_sum[:, at] = jnp.sum(lanes.T, axis=0, keepdims=True)
    sums[y] = own_sum[...]

    for copy in small:
        copy.wait()
    part[...] = (w_v[...] * g_v[...]).astype(jnp.bfloat16).astype(jnp.float32)

    @pl.when(y != GATE)
    def _():
        pl.semaphore_wait(barrier, zero - 1)

    @pl.when(y == HERALD)
    def _():
        signal(ready, {"zero": GATE})

    @pl.when(y == GATE)
    def _():
        pl.semaphore_wait(ready, 1)

    left, right = lax.rem(y + zero - 1, zero), lax.rem(y + 1, zero)

    def by_ring(act):
        for late, count in ((True, LEAST), (False, EARLY)):

            @pl.when((bank == 0) == late)
            def _(count=count):
                act(count)

    def send_early(way, count):
        first = 0 if way == 0 else rows - count
        return remote(
            merged.at[pl.ds(first, count)], early.at[way, pl.ds(0, count)], early_send, early_recv.at[way],
            {"zero": right if way == 0 else left},
        )

    def start_early(count):
        for way in (0, 1) if count else ():
            send_early(way, count).start()

    for k in (4, 3, 5, 2, 6, 1, 7):
        remote(own_sum, sums.at[y], sum_send, sum_recv, {"zero": lax.rem(y + k, zero)}).start()
    by_ring(start_early)
    for k in range(1, zero):
        remote(part, column.at[y], part_send, part_recv, {"zero": lax.rem(y + k, zero)}).start()
    own_part = pltpu.make_async_copy(part, column.at[y], local_sem)
    own_part.start()

    others = [at_core(1)]
    others += [at_x(k) for k in range(1, X)]
    others += [at_z(k) for k in range(1, depth)]

    @pl.when(y == GATE)
    def _():
        for peer in others:
            signal(barrier, {"bank": peer})

    arrived(sums.at[pl.ds(0, zero - 1)], sum_recv)
    total = jnp.sqrt(jnp.sum(sums[...], axis=0))
    scale[...] = total
    inverse = 1.0 / total

    def columns(owner):
        return pl.ds(pl.multiple_of(owner * cols, cols), cols)

    def narrow(source, start, count, owner):
        block = start // BLOCK * BLOCK
        tall = jnp.broadcast_to(inverse[:, block : block + BLOCK], (BLOCK, BLOCK)).T
        wide = jnp.concatenate([tall[start - block : start - block + count]] * (cols // 128), axis=1)
        final[start : start + count, columns(owner)] = (source[...] * wide).astype(jnp.bfloat16)

    def ring(way, hop, place, first=0, last=half):
        if way == 0:
            start = place * half + first
        else:
            start = rows - place * half - last
        owner = lax.rem(y + (zero - hop if way == 0 else hop), zero)
        at = final.at[pl.ds(start, last - first), columns(owner)]
        return remote(
            at, at, ring_send.at[way], ring_recv.at[way, hop * HALVES + place],
            {"zero": right if way == 0 else left},
        )

    done, waiting = set(), None

    def own(start, stop):
        for i in range(start // BLOCK, -(-stop // BLOCK)):
            if i not in done:
                done.add(i)
                narrow(merged.at[pl.ds(i * BLOCK, BLOCK)], i * BLOCK, BLOCK, y)

    def send_own(way, place, first, last):
        if (place, first) == (0, LEAST):
            by_ring(lambda count: ring(way, 0, place, count, last).start())
        else:
            ring(way, 0, place, first, last).start()

    for place, first, last in ((0, LEAST, FIRST), (0, FIRST, half), (1, 0, FIRST), (1, FIRST, half)):
        for way in (0, 1):
            start, stop = place * half + first, place * half + last
            own(*((start, stop) if way == 0 else (rows - stop, rows - start)))
            if waiting:
                send_own(*waiting)
            waiting = (way, place, first, last)
    own(0, rows)

    def take_early(count):
        for way in (0, 1) if count else ():
            send_early(way, count).wait_recv()
            first = 0 if way == 0 else rows - count
            for i in range(0, count, 64):
                narrow(early.at[way, pl.ds(i, 64)], first + i, 64, left if way == 0 else right)

    by_ring(take_early)
    send_own(*waiting)

    stages = [
        (bank, 1, [at_core(1)]),
        (bank - core, CORES, [at_x(k) for k in range(1, X)]),
        (chip_z * X * CORES, X * CORES, [at_z(k) for k in range(1, depth)]),
    ]

    def table_stage(s):
        if s:
            _, count, peers = stages[s - 1]
            arrived(table.at[pl.ds(0, count * len(peers))], table_recv.at[s - 1])
        else:
            own_part.wait()
            arrived(column.at[pl.ds(0, zero - 1)], part_recv)
            own_row = pltpu.make_async_copy(column, table.at[bank], local_sem)
            own_row.start()
            own_row.wait()
        if s < len(stages):
            first, count, peers = stages[s]
            at = table.at[pl.ds(first, count)]
            for peer in peers:
                remote(at, at, table_send, table_recv.at[s], {"bank": peer}).start()
        else:
            width = part.shape[1]
            for j in range(zero):
                router[:, j * width : (j + 1) * width] = table[:, j, 0, :].astype(jnp.bfloat16)

    def open_gate():
        @pl.when(y == GATE)
        def _():
            pl.semaphore_wait(barrier, len(others))
            for k in range(1, zero):
                signal(opened, {"zero": (GATE + k) % zero})

    def pass_gate():
        @pl.when(y != GATE)
        def _():
            pl.semaphore_wait(opened, 1)

        table_stage(0)

    between = {
        (1, 0): open_gate,
        (1, 1): pass_gate,
        (2, 0): lambda: table_stage(1),
        (2, 1): lambda: table_stage(2),
        (3, 0): lambda: table_stage(3),
    }
    for hop in (1, 2, 3, 4):
        for place in range(HALVES if hop < 4 else 1):
            for way in (0, 1):
                if (hop, place) == (1, 0):
                    by_ring(lambda count: ring(way, 0, 0, count).wait_recv())
                else:
                    ring(way, hop - 1, place).wait_recv()
                if hop < 3 or (hop == 3 and place == 0):
                    ring(way, hop, place).start()
            if (hop, place) in between:
                between[hop, place]()

    def ring_left(count):
        for way in (0, 1):
            arrived(final.at[pl.ds(0, (rows * 7 // 2 - count) // 4), pl.ds(0, 4 * cols)], ring_send.at[way])
        if count:
            arrived(early.at[pl.ds(0, 2 * count // EARLY)], early_send)

    by_ring(ring_left)
    arrived(sums.at[pl.ds(0, zero - 1)], sum_send)
    arrived(column.at[pl.ds(0, zero - 1)], part_send)
    arrived(table.at[pl.ds(0, table.shape[0] - 1)], table_send)


def write(final, scale, router, final_out, scale_out, router_out, sem):
    copies = [
        pltpu.make_async_copy(final, final_out, sem.at[0]),
        pltpu.make_async_copy(router, router_out, sem.at[1]),
        pltpu.make_async_copy(scale, scale_out, sem.at[2]),
    ]
    for copy in copies:
        copy.start()
    for copy in copies:
        copy.wait()


def body(master_down, second_down, router_weight, router_gain):
    _, rows, cols = master_down.shape
    width = router_weight.shape[0]
    zero, banks = lax.axis_size("zero"), lax.axis_size("bank")
    f32, vmem, dma = jnp.float32, pltpu.VMEM, pltpu.SemaphoreType.DMA
    args = (
        master_down.reshape(rows, cols),
        second_down.reshape(rows, cols),
        router_weight.reshape(1, width),
        router_gain.reshape(1, width),
    )
    results = pl.pallas_call(
        kernel,
        out_shape=(
            jax.ShapeDtypeStruct((rows, zero * cols), jnp.bfloat16),
            jax.ShapeDtypeStruct((1, rows), f32),
            jax.ShapeDtypeStruct((banks, zero * width), jnp.bfloat16),
        ),
        in_specs=[pl.BlockSpec(memory_space=pltpu.HBM)] * 4,
        out_specs=[pl.BlockSpec(memory_space=vmem)] * 3,
        scratch_shapes=[
            vmem((rows, cols), f32),
            vmem((rows, cols), jnp.bfloat16),
            vmem((1, rows), f32),
            vmem((zero, 1, rows), f32),
            vmem((1, width), f32),
            vmem((1, width), f32),
            vmem((1, width), f32),
            vmem((zero, 1, width), f32),
            vmem((banks, zero, 1, width), f32),
            vmem((2, EARLY, cols), f32),
            pltpu.SemaphoreType.REGULAR,
            pltpu.SemaphoreType.REGULAR,
            dma((2,)),
            dma((2,)),
            dma(()),
            dma(()),
            dma(()),
            dma(()),
            dma(()),
            dma(()),
            dma((3,)),
            dma(()),
            dma((2,)),
            dma((2,)),
            dma((2, 3 * HALVES + 1)),
        ],
        compiler_params=pltpu.CompilerParams(
            collective_id=0, has_side_effects=True, vmem_limit_bytes=40 * 2**20
        ),
        name="gather",
    )(*map(in_hbm, args))
    final, scale, router = pl.pallas_call(
        write,
        out_shape=tuple(jax.ShapeDtypeStruct(x.shape, x.dtype) for x in results),
        in_specs=[pl.BlockSpec(memory_space=pl.ANY)] * 3,
        out_specs=[pl.BlockSpec(memory_space=pl.ANY)] * 3,
        scratch_shapes=[dma((3,))],
        compiler_params=pltpu.CompilerParams(vmem_limit_bytes=2**20),
        name="write",
    )(*(pltpu.with_memory_space_constraint(x, vmem) for x in results))
    return final.reshape(1, rows, zero * cols), scale, router.T


def in_hbm(value):
    return pltpu.with_memory_space_constraint(value, pltpu.HBM)


def solution(mesh):
    return jax.shard_map(
        body,
        mesh=mesh,
        in_specs=(P("bank", None, "zero"), P("bank", None, "zero"), P("zero", "bank"), P("zero")),
        out_specs=(P("bank", None, None), P("bank", None), P()),
        check_vma=False,
    )
```

```python
import jax
import jax.numpy as jnp
from jax import lax
from jax.experimental import pallas as pl
from jax.experimental.pallas import tpu as pltpu
from jax.sharding import PartitionSpec as P

MESH = pl.DeviceIdType.MESH
BLOCK = 128
HALVES = 2
FIRST = 352
LOADS = 4
EARLY = 128
LEAST = 0
GATE, HERALD = 7, 6
X, CORES = 4, 2


def kernel(
    master, second, weight, gain,
    final, scale, router,
    merged, added, own_sum, sums, w_v, g_v, part, column, table, early,
    ready, opened, load_sem, small_sem, local_sem,
    sum_send, sum_recv, part_send, part_recv, table_send, table_recv,
    early_send, early_recv, ring_send, ring_recv,
):
    rows, cols = merged.shape
    zero = lax.axis_size("zero")
    blocks, half = rows // BLOCK, rows // HALVES
    y, bank = lax.axis_index("zero"), lax.axis_index("bank")
    chip_z, chip_x = bank // (X * CORES), lax.rem(bank // CORES, X)
    depth = lax.axis_size("bank") // (X * CORES)
    core = lax.rem(bank, CORES)

    def at_core(k):
        return bank - core + lax.rem(core + k, CORES)

    def at_x(k):
        return (chip_z * X + lax.rem(chip_x + k, X)) * CORES + core

    def at_z(k):
        return (lax.rem(chip_z + k, depth) * X + chip_x) * CORES + core

    def signal(sem, peer):
        pl.semaphore_signal(sem, inc=1, device_id=peer, device_id_type=MESH)

    def arrived(ref, sem):
        pltpu.make_async_copy(ref, ref, sem).wait()

    def remote(source, target, send_sem, recv_sem, peer):
        return pltpu.make_async_remote_copy(
            source, target, send_sem, recv_sem, device_id=peer, device_id_type=MESH
        )

    barrier = pltpu.get_barrier_semaphore()
    for k in (4, 3, 5, 2, 6, 1, 7):
        peer = lax.rem(y + k, zero)

        @pl.when(peer != GATE)
        def _(peer=peer):
            signal(barrier, {"zero": peer})

    step = rows // LOADS
    for i in range(LOADS):
        at = pl.ds(i * step, step)
        pltpu.make_async_copy(master.at[at], merged.at[at], load_sem.at[0]).start()
        pltpu.make_async_copy(second.at[at], added.at[at], load_sem.at[1]).start()
    small = (
        pltpu.make_async_copy(weight, w_v, small_sem.at[0]),
        pltpu.make_async_copy(gain, g_v, small_sem.at[1]),
    )
    for copy in small:
        copy.start()

    arrived(merged, load_sem.at[0])
    arrived(added, load_sem.at[1])
    for i in range(blocks):
        at = pl.ds(i * BLOCK, BLOCK)
        value = merged[at] + added[at].astype(jnp.float32)
        merged[at] = value
        square = value * value
        lanes = square[:, :128]
        for j in range(128, cols, 128):
            lanes = lanes + square[:, j : j + 128]
        own_sum[:, at] = jnp.sum(lanes.T, axis=0, keepdims=True)
    sums[y] = own_sum[...]

    for copy in small:
        copy.wait()
    part[...] = (w_v[...] * g_v[...]).astype(jnp.bfloat16).astype(jnp.float32)

    @pl.when(y != GATE)
    def _():
        pl.semaphore_wait(barrier, zero - 1)

    @pl.when(y == HERALD)
    def _():
        signal(ready, {"zero": GATE})

    @pl.when(y == GATE)
    def _():
        pl.semaphore_wait(ready, 1)

    left, right = lax.rem(y + zero - 1, zero), lax.rem(y + 1, zero)

    def by_ring(act):
        for late, count in ((True, LEAST), (False, EARLY)):

            @pl.when((bank == 0) == late)
            def _(count=count):
                act(count)

    def send_early(way, count):
        first = 0 if way == 0 else rows - count
        return remote(
            merged.at[pl.ds(first, count)], early.at[way, pl.ds(0, count)], early_send, early_recv.at[way],
            {"zero": right if way == 0 else left},
        )

    def start_early(count):
        for way in (0, 1) if count else ():
            send_early(way, count).start()

    for k in (4, 3, 5, 2, 6, 1, 7):
        remote(own_sum, sums.at[y], sum_send, sum_recv, {"zero": lax.rem(y + k, zero)}).start()
    by_ring(start_early)
    for k in range(1, zero):
        remote(part, column.at[y], part_send, part_recv, {"zero": lax.rem(y + k, zero)}).start()
    own_part = pltpu.make_async_copy(part, column.at[y], local_sem)
    own_part.start()

    others = [at_core(1)]
    others += [at_x(k) for k in range(1, X)]
    others += [at_z(k) for k in range(1, depth)]

    @pl.when(y == GATE)
    def _():
        for peer in others:
            signal(barrier, {"bank": peer})

    arrived(sums.at[pl.ds(0, zero - 1)], sum_recv)
    total = jnp.sqrt(jnp.sum(sums[...], axis=0))
    scale[...] = total
    inverse = 1.0 / total

    def columns(owner):
        return pl.ds(pl.multiple_of(owner * cols, cols), cols)

    def narrow(source, start, count, owner):
        block = start // BLOCK * BLOCK
        tall = jnp.broadcast_to(inverse[:, block : block + BLOCK], (BLOCK, BLOCK)).T
        wide = jnp.concatenate([tall[start - block : start - block + count]] * (cols // 128), axis=1)
        final[start : start + count, columns(owner)] = (source[...] * wide).astype(jnp.bfloat16)

    def ring(way, hop, place, first=0, last=half):
        if way == 0:
            start = place * half + first
        else:
            start = rows - place * half - last
        owner = lax.rem(y + (zero - hop if way == 0 else hop), zero)
        at = final.at[pl.ds(start, last - first), columns(owner)]
        return remote(
            at, at, ring_send.at[way], ring_recv.at[way, hop * HALVES + place],
            {"zero": right if way == 0 else left},
        )

    def send_own(way, place, first, last):
        if (place, first) == (0, LEAST):
            by_ring(lambda count: ring(way, 0, place, count, last).start())
        else:
            ring(way, 0, place, first, last).start()

    done, queue = set(), []

    def follow():
        while queue:
            send_own(*queue.pop(0))

    def own(start, stop):
        for i in range(start // BLOCK, -(-stop // BLOCK)):
            if i not in done:
                done.add(i)
                narrow(merged.at[pl.ds(i * BLOCK, BLOCK)], i * BLOCK, BLOCK, y)
                follow()

    for place, first, last in ((0, LEAST, FIRST), (0, FIRST, half), (1, 0, FIRST), (1, FIRST, half)):
        for way in (0, 1):
            start, stop = place * half + first, place * half + last
            own(*((start, stop) if way == 0 else (rows - stop, rows - start)))
            queue.append((way, place, first, last))
    own(0, rows)

    def take_early(count):
        for way in (0, 1) if count else ():
            send_early(way, count).wait_recv()
            first = 0 if way == 0 else rows - count
            for i in range(0, count, 64):
                narrow(early.at[way, pl.ds(i, 64)], first + i, 64, left if way == 0 else right)

    by_ring(take_early)
    follow()

    stages = [
        (bank, 1, [at_core(1)]),
        (bank - core, CORES, [at_x(k) for k in range(1, X)]),
        (chip_z * X * CORES, X * CORES, [at_z(k) for k in range(1, depth)]),
    ]

    def table_stage(s):
        if s:
            _, count, peers = stages[s - 1]
            arrived(table.at[pl.ds(0, count * len(peers))], table_recv.at[s - 1])
        else:
            own_part.wait()
            arrived(column.at[pl.ds(0, zero - 1)], part_recv)
            own_row = pltpu.make_async_copy(column, table.at[bank], local_sem)
            own_row.start()
            own_row.wait()
        if s < len(stages):
            first, count, peers = stages[s]
            at = table.at[pl.ds(first, count)]
            for peer in peers:
                remote(at, at, table_send, table_recv.at[s], {"bank": peer}).start()
        else:
            width = part.shape[1]
            for j in range(zero):
                router[:, j * width : (j + 1) * width] = table[:, j, 0, :].astype(jnp.bfloat16)

    def open_gate():
        @pl.when(y == GATE)
        def _():
            pl.semaphore_wait(barrier, len(others))
            for k in range(1, zero):
                signal(opened, {"zero": (GATE + k) % zero})

    def pass_gate():
        @pl.when(y != GATE)
        def _():
            pl.semaphore_wait(opened, 1)

        table_stage(0)

    between = {
        (1, 0): open_gate,
        (1, 1): pass_gate,
        (2, 0): lambda: table_stage(1),
        (2, 1): lambda: table_stage(2),
        (3, 0): lambda: table_stage(3),
    }
    for hop in (1, 2, 3, 4):
        for place in range(HALVES if hop < 4 else 1):
            for way in (0, 1):
                if (hop, place) == (1, 0):
                    by_ring(lambda count: ring(way, 0, 0, count).wait_recv())
                else:
                    ring(way, hop - 1, place).wait_recv()
                if hop < 3 or (hop == 3 and place == 0):
                    ring(way, hop, place).start()
            if (hop, place) in between:
                between[hop, place]()

    def ring_left(count):
        for way in (0, 1):
            arrived(final.at[pl.ds(0, (rows * 7 // 2 - count) // 4), pl.ds(0, 4 * cols)], ring_send.at[way])
        if count:
            arrived(early.at[pl.ds(0, 2 * count // EARLY)], early_send)

    by_ring(ring_left)
    arrived(sums.at[pl.ds(0, zero - 1)], sum_send)
    arrived(column.at[pl.ds(0, zero - 1)], part_send)
    arrived(table.at[pl.ds(0, table.shape[0] - 1)], table_send)


def write(final, scale, router, final_out, scale_out, router_out, sem):
    copies = [
        pltpu.make_async_copy(final, final_out, sem.at[0]),
        pltpu.make_async_copy(router, router_out, sem.at[1]),
        pltpu.make_async_copy(scale, scale_out, sem.at[2]),
    ]
    for copy in copies:
        copy.start()
    for copy in copies:
        copy.wait()


def body(master_down, second_down, router_weight, router_gain):
    _, rows, cols = master_down.shape
    width = router_weight.shape[0]
    zero, banks = lax.axis_size("zero"), lax.axis_size("bank")
    f32, vmem, dma = jnp.float32, pltpu.VMEM, pltpu.SemaphoreType.DMA
    args = (
        master_down.reshape(rows, cols),
        second_down.reshape(rows, cols),
        router_weight.reshape(1, width),
        router_gain.reshape(1, width),
    )
    results = pl.pallas_call(
        kernel,
        out_shape=(
            jax.ShapeDtypeStruct((rows, zero * cols), jnp.bfloat16),
            jax.ShapeDtypeStruct((1, rows), f32),
            jax.ShapeDtypeStruct((banks, zero * width), jnp.bfloat16),
        ),
        in_specs=[pl.BlockSpec(memory_space=pltpu.HBM)] * 4,
        out_specs=[pl.BlockSpec(memory_space=vmem)] * 3,
        scratch_shapes=[
            vmem((rows, cols), f32),
            vmem((rows, cols), jnp.bfloat16),
            vmem((1, rows), f32),
            vmem((zero, 1, rows), f32),
            vmem((1, width), f32),
            vmem((1, width), f32),
            vmem((1, width), f32),
            vmem((zero, 1, width), f32),
            vmem((banks, zero, 1, width), f32),
            vmem((2, EARLY, cols), f32),
            pltpu.SemaphoreType.REGULAR,
            pltpu.SemaphoreType.REGULAR,
            dma((2,)),
            dma((2,)),
            dma(()),
            dma(()),
            dma(()),
            dma(()),
            dma(()),
            dma(()),
            dma((3,)),
            dma(()),
            dma((2,)),
            dma((2,)),
            dma((2, 3 * HALVES + 1)),
        ],
        compiler_params=pltpu.CompilerParams(
            collective_id=0, has_side_effects=True, vmem_limit_bytes=40 * 2**20
        ),
        name="gather",
    )(*map(in_hbm, args))
    final, scale, router = pl.pallas_call(
        write,
        out_shape=tuple(jax.ShapeDtypeStruct(x.shape, x.dtype) for x in results),
        in_specs=[pl.BlockSpec(memory_space=pl.ANY)] * 3,
        out_specs=[pl.BlockSpec(memory_space=pl.ANY)] * 3,
        scratch_shapes=[dma((3,))],
        compiler_params=pltpu.CompilerParams(vmem_limit_bytes=2**20),
        name="write",
    )(*(pltpu.with_memory_space_constraint(x, vmem) for x in results))
    return final.reshape(1, rows, zero * cols), scale, router.T


def in_hbm(value):
    return pltpu.with_memory_space_constraint(value, pltpu.HBM)


def solution(mesh):
    return jax.shard_map(
        body,
        mesh=mesh,
        in_specs=(P("bank", None, "zero"), P("bank", None, "zero"), P("zero", "bank"), P("zero")),
        out_specs=(P("bank", None, None), P("bank", None), P()),
        check_vma=False,
    )
```
